32 devices in a mesh: gx: 8 (over y, x, core), gy: 4 (over z).
Axes of the slice: x: 2, y: 2, z: 4, core: 2. Of those that a mesh axis runs over, the one named last changes fastest.
Arguments:
- candidate_owner: int32 [256, 512, 1], P(('gx', 'gy')), may hold values from 0 to 31; in each aligned block of 4096 rows (0 to 4095, 4096 to 8191, ..., all dimensions but the last counted through in order) at most 256 rows name the same one
- candidate_row: int32 [256, 512], P(('gx', 'gy')), may hold values from 0 to 78335
- item_table: bfloat16 [2506752, 128], P(('gx', 'gy')), may hold values from -6 to 6
- w_in: bfloat16 [128, 512], replicated, may hold values from -0.5 to 0.5
- w_qkv: bfloat16 [1, 512, 1536], replicated, may hold values from -0.25 to 0.25
- w_out: bfloat16 [1, 512, 512], replicated, may hold values from -0.25 to 0.25
- w_up: bfloat16 [1, 512, 1024], replicated, may hold values from -0.25 to 0.25
- w_down: bfloat16 [1, 1024, 512], replicated, may hold values from -0.1875 to 0.1875
- norm_gains: float32 [1, 2, 512], replicated, may hold values from 0.25 to 1.75
- final_gain: float32 [512], replicated, may hold values from 0.25 to 1.75
- w_score: bfloat16 [512], replicated, may hold values from -0.25 to 0.25
Outputs:
- log_probs: float32 [256, 512], P(('gx', 'gy'))
The draws below stay inside these ranges and needn't reach their ends.
Inputs may be any that keep to these rules, and one draw needn't show every extreme that they name: `candidate_owner`: among the candidates of one device's 8 slates no shard is named more than 256 times, a bound that some block reaches.
All inputs are finite; a program needn't handle non-finite values.
Results may differ from the reference program's by a relative error of at most 0.0007.
Values may be sent and summed in bfloat16 or wider, within the bound.
No kernel may reach another device: no remote copies, remote signals or barrier semaphores. Data moves between devices by JAX's collectives and lax.ppermute only.
A program may use at most 128 MiB of HBM per device.

```python
import math
import jax
import jax.numpy as jnp
import numpy as np
from jax import lax

SLATE_LEN = 512
SLATES_DEV = 8
SLATES = 256
EMB = 128
ROWS_DEV = 78336
ROWS = 2506752
D = 512
HEADS = 8
FF = 1024
LAYERS = 1
CAP = 256
N_GX = 8
N_GY = 4


def set_ends(values, rng, smallest, largest):
    dims = values.shape
    place = [jax.random.randint(jax.random.fold_in(rng, axis), (), 0, dims[axis]) for axis in range(len(dims))]
    values = values.at[tuple(place)].set(smallest)
    longest = dims.index(max(dims))
    place[longest] = (place[longest] + 1) % dims[longest]
    return values.at[tuple(place)].set(largest)


def shard_levels(stream_key, shape, split, smallest, high):
    level, own = 1.0, jax.random.fold_in(stream_key, 6)
    for position, shards_of in split:
        steps = jnp.exp(jax.random.uniform(jax.random.fold_in(own, position), (shards_of,), jnp.float32, smallest / len(split), high / len(split)))
        level = level * jnp.repeat(steps, shape[position] // shards_of).reshape([-1 if axis == position else 1 for axis in range(len(shape))])
    return level


def wide_ids(key, dims, number_of, slope):
    portions = [min(1 << octave, number_of + 1 - (1 << octave)) * (1 << 20) // math.isqrt((1 << octave) ** slope) + 1 for octave in range((number_of + 1).bit_length()) if 1 << octave <= number_of]
    spread = 1 + sum(portions) // (1 << 30)
    listing = np.cumsum(np.array([max(1, weight // spread) for weight in portions]))
    pick = jax.random.randint(jax.random.fold_in(key, 1), dims, 0, int(listing[len(portions) - 1]))
    start = jnp.left_shift(1, jnp.searchsorted(jnp.asarray(listing, jnp.int32), pick, side="right").astype(jnp.int32))
    grade = start - 1 + jax.random.randint(jax.random.fold_in(key, 4), dims, 0, 1 << 30) % jnp.minimum(start, number_of + 1 - start)
    return jax.random.permutation(jax.random.fold_in(key, 2), number_of)[grade].astype(jnp.int32)


def deal_out(rng, own, number, rows, number_of, top, bound, skew):
    sequence = jax.random.permutation(rng, number_of)
    packed, common = load_shares(number_of, rows * top, bound, skew, True), load_shares(number_of, rows * top, bound, skew, False)
    places = jnp.arange(number_of)

    def named(lengths, turn):
        used = int((lengths > 0).sum())
        fixed = max(1, used // 4)
        moved = fixed + (places - fixed + turn * (used - fixed)) % max(1, number_of - fixed)
        return jnp.zeros((number_of,), jnp.int32).at[sequence[jnp.where(places < fixed, places, moved)]].set(jnp.asarray(lengths, jnp.int32))

    lengths = jnp.where(number % 4 == 0, named(packed, number // 4), named(common, number - number // 4 - 1))
    mixed = jax.random.permutation(jax.random.fold_in(own, 3), number_of)
    source_of, sink = mixed[0:number_of // 2 * 2:2], mixed[1:number_of // 2 * 2:2]
    room = jnp.minimum(lengths[source_of] - 1, bound - lengths[sink]) // 2
    room = jnp.where((source_of == sequence[0]) | (sink == sequence[0]) | (lengths[sink] == 0), 0, jnp.maximum(room, 0))
    moved = jax.random.randint(jax.random.fold_in(own, 4), (number_of // 2,), 0, 1 << 20) % (room + 1)
    lengths = lengths.at[source_of].add(-moved).at[sink].add(moved)
    members = jnp.searchsorted(jnp.cumsum(lengths), jnp.arange(rows * top), side="right").astype(jnp.int32)
    grid = members.reshape(top, rows).T
    grid = grid[jax.random.permutation(jax.random.fold_in(own, 1), rows)]
    turn = jax.random.randint(jax.random.fold_in(own, 2), (rows, 1), 0, top)
    return jnp.take_along_axis(grid, (jnp.arange(top)[None, :] + turn) % top, axis=1)


def load_shares(amount, total, limit, lean, full):
    portions = [(1 << 20) // math.isqrt(standing ** lean) + 1 for standing in range(1, amount + 1)]
    largest = limit if full else min(limit, max(-(-total // amount), total * portions[0] // sum(portions)))
    least = 1 if total - largest >= amount - 1 else 0
    holding, rest = [largest] + [least] * (amount - 1), total - largest - least * (amount - 1)
    while rest > 0:
        free = [i for i in range(1, amount) if holding[i] < largest] or [i for i in range(1, amount) if holding[i] < limit]
        pool, budget = sum([portions[i] for i in free]), rest
        for i in free:
            addition = min(limit - holding[i], max(1, budget * portions[i] // pool), rest)
            holding[i] = holding[i] + addition
            rest = rest - addition
    return np.array(holding)


def normal_values(own_key, extent, scale, most, pieces=(), dtype=jnp.bfloat16):
    factor_of = shard_levels(own_key, extent, pieces, -0.22, 0.18) if pieces else 1.0
    drawn = jax.random.normal(own_key, extent, jnp.float32) * scale * factor_of
    return jnp.minimum(jnp.maximum(drawn, -most), most).astype(dtype)


def setup_inputs(seed: int = 0) -> dict:
    arg_keys = jax.random.split(jax.random.key(seed), 12)
    candidate_owner_keys = jax.random.split(jax.random.fold_in(arg_keys[0], 1), SLATES * SLATE_LEN // (SLATES_DEV * SLATE_LEN))
    candidate_owner_turns = jax.random.permutation(jax.random.fold_in(arg_keys[0], 3), SLATES * SLATE_LEN // (SLATES_DEV * SLATE_LEN))
    candidate_owner = jax.vmap(lambda own, number: deal_out(jax.random.fold_in(arg_keys[0], 2), own, number, SLATES_DEV * SLATE_LEN, N_GX * N_GY, 1, CAP, 2))(candidate_owner_keys, candidate_owner_turns).reshape((SLATES, SLATE_LEN, 1))
    candidate_row = set_ends(wide_ids(arg_keys[1], (SLATES, SLATE_LEN), ROWS_DEV, 2), jax.random.fold_in(arg_keys[1], 3), 0, ROWS_DEV - 1).astype(jnp.int32)
    item_table = normal_values(arg_keys[2], (ROWS, EMB), 1.0, 6.0, ((0, 32),))
    w_in = normal_values(arg_keys[3], (EMB, D), EMB ** -0.5, 0.5)
    w_qkv = normal_values(arg_keys[4], (LAYERS, D, 3 * D), D ** -0.5, 0.25)
    w_out = normal_values(arg_keys[5], (LAYERS, D, D), D ** -0.5, 0.25)
    w_up = normal_values(arg_keys[6], (LAYERS, D, FF), D ** -0.5, 0.25)
    w_down = normal_values(arg_keys[7], (LAYERS, FF, D), FF ** -0.5, 0.1875)
    norm_gains = jnp.clip(1.0 + 0.15 * jax.random.normal(arg_keys[8], (LAYERS, 2, D), jnp.float32), 0.25, 1.75)
    final_gain = jnp.clip(1.0 + 0.15 * jax.random.normal(arg_keys[9], (D,), jnp.float32), 0.25, 1.75)
    w_score = normal_values(arg_keys[10], (D,), D ** -0.5, 0.25)
    return dict(candidate_owner=candidate_owner, candidate_row=candidate_row, item_table=item_table, w_in=w_in, w_qkv=w_qkv, w_out=w_out, w_up=w_up, w_down=w_down, norm_gains=norm_gains, final_gain=final_gain, w_score=w_score)


def layer_norm(values, gain):
    mean = lax.optimization_barrier(jnp.mean(values, axis=-1, keepdims=True))
    centred = values - mean
    variance = lax.optimization_barrier(jnp.mean(centred * centred, axis=-1, keepdims=True))
    return centred * lax.rsqrt(variance + 1e-05) * gain

def score_slates(emb, w_in, w_qkv, w_out, w_up, w_down, norm_gains, final_gain, w_score):
    slates, length, width = emb.shape
    model = w_in.shape[1]
    head_dim = model // HEADS
    resid = jnp.dot(emb.reshape(slates * length, width), w_in, preferred_element_type=jnp.float32)
    for layer in range(LAYERS):
        normed = layer_norm(resid, norm_gains[layer, 0]).astype(jnp.bfloat16)
        qkv = jnp.dot(normed, w_qkv[layer], preferred_element_type=jnp.float32).astype(jnp.bfloat16)
        qkv = qkv.reshape(slates, length, 3, HEADS, head_dim)
        query = qkv[:, :, 0].astype(jnp.float32)
        keys = qkv[:, :, 1].astype(jnp.float32)
        values = qkv[:, :, 2].astype(jnp.float32)
        scores = jnp.einsum('bqhd,bkhd->bhqk', query, keys) * head_dim ** (-0.5)
        probs = jax.nn.softmax(scores, axis=-1).astype(jnp.bfloat16)
        mixed = jnp.einsum('bhqk,bkhd->bqhd', probs.astype(jnp.float32), values)
        mixed = mixed.astype(jnp.bfloat16).reshape(slates * length, model)
        resid = resid + jnp.dot(mixed, w_out[layer], preferred_element_type=jnp.float32)
        normed = layer_norm(resid, norm_gains[layer, 1]).astype(jnp.bfloat16)
        inner = jax.nn.gelu(jnp.dot(normed, w_up[layer], preferred_element_type=jnp.float32)).astype(jnp.bfloat16)
        resid = resid + jnp.dot(inner, w_down[layer], preferred_element_type=jnp.float32)
    final = layer_norm(resid, final_gain)
    logits = lax.optimization_barrier(jnp.sum(final * w_score.astype(jnp.float32)[None, :], axis=-1))
    return jax.nn.log_softmax(logits.reshape(slates, length), axis=-1)

def reference(candidate_owner, candidate_row, item_table, w_in, w_qkv, w_out, w_up, w_down, norm_gains, final_gain, w_score):
    item = (candidate_owner[:, :, 0] * ROWS_DEV + candidate_row).astype(jnp.int32)
    emb = jnp.take(item_table, item.reshape(-1), axis=0)
    emb = emb.reshape(N_GX * N_GY * SLATES_DEV, 1, SLATE_LEN, EMB)

    def one_group(block):
        return score_slates(block, w_in, w_qkv, w_out, w_up, w_down, norm_gains, final_gain, w_score)
    scored = lax.map(one_group, emb)
    return scored.reshape(SLATES, SLATE_LEN)
```

```python
import functools

import jax
import jax.numpy as jnp
from jax import lax
from jax.experimental import pallas as pl
from jax.experimental.pallas import tpu as pltpu
from jax.sharding import PartitionSpec as P

HEADS = 8


def dot(a, b):
    return jnp.dot(a, b, preferred_element_type=jnp.float32)


def dot_nt(a, b):
    return lax.dot_general(a, b, (((1,), (1,)), ((), ())), preferred_element_type=jnp.float32)


def layer_norm(values, gain):
    mean = jnp.mean(values, axis=-1, keepdims=True)
    centred = values - mean
    variance = jnp.mean(centred * centred, axis=-1, keepdims=True)
    return centred * lax.rsqrt(variance + 1e-05) * gain


def plan_kernel(owner_ref, row_ref, outgoing_ref, position_ref, *, shards, capacity):
    slates, length = row_ref.shape
    tri = (
        lax.broadcasted_iota(jnp.int32, (length, length), 0)
        <= lax.broadcasted_iota(jnp.int32, (length, length), 1)
    ).astype(jnp.float32).astype(jnp.bfloat16)
    shard_ids = lax.broadcasted_iota(jnp.int32, (shards, length), 0)
    slot_ids = lax.broadcasted_iota(jnp.int32, (capacity, length), 0)
    before = jnp.zeros((shards, 1), jnp.float32)
    acc = jnp.zeros((3 * shards, capacity), jnp.float32)
    for s in range(slates):
        owner = owner_ref[s : s + 1, :]
        row = row_ref[s : s + 1, :]
        onehot = (owner == shard_ids).astype(jnp.float32)
        counts = dot(onehot.astype(jnp.bfloat16), tri) + before
        before = counts[:, length - 1 :]
        slot = (jnp.sum(counts * onehot, axis=0, keepdims=True) - 1.0).astype(jnp.int32)
        position_ref[s : s + 1, :] = owner * capacity + slot
        digits = [(row & 255), ((row >> 8) & 255), (row >> 16)]
        lhs = jnp.concatenate(
            [onehot * digit.astype(jnp.float32) for digit in digits], axis=0
        ).astype(jnp.bfloat16)
        chosen = (slot == slot_ids).astype(jnp.float32).astype(jnp.bfloat16)
        acc = acc + dot_nt(lhs, chosen)
    parts = acc.astype(jnp.int32)
    outgoing_ref[...] = (
        parts[:shards] + (parts[shards : 2 * shards] << 8) + (parts[2 * shards :] << 16)
    )


def plan(owner, row_index, shards, capacity):
    return pl.pallas_call(
        functools.partial(plan_kernel, shards=shards, capacity=capacity),
        out_shape=(
            jax.ShapeDtypeStruct((shards, capacity), jnp.int32),
            jax.ShapeDtypeStruct(row_index.shape, jnp.int32),
        ),
        name="plan",
    )(owner, row_index)


def slate_kernel(
    position_ref,
    rows_ref,
    w_in_ref,
    w_qkv_ref,
    w_out_ref,
    w_up_ref,
    w_down_ref,
    gains_ref,
    final_gain_ref,
    w_score_ref,
    out_ref,
    table_ref,
    emb_ref,
    mixed_ref,
):
    slate = pl.program_id(0)
    length = emb_ref.shape[0]
    model = w_in_ref.shape[1]
    head_dim = model // HEADS
    pair = 2 * head_dim

    @pl.when(slate == 0)
    def _():
        table_ref[...] = rows_ref[...].astype(jnp.float32)

    def pick(group, carry):
        for j in range(16):
            r = group * 16 + j
            p = position_ref[slate * length + r]
            emb_ref[pl.ds(r, 1), :] = table_ref[pl.ds(p, 1), :]
        return carry

    lax.fori_loop(0, length // 16, pick, 0)

    resid = dot(emb_ref[...].astype(jnp.bfloat16), w_in_ref[...])
    normed = layer_norm(resid, gains_ref[0:1, :]).astype(jnp.bfloat16)
    lane = lax.broadcasted_iota(jnp.int32, (1, pair), 1)
    low = lane < head_dim
    scale = head_dim ** (-0.5)
    low_scale = jnp.where(low, scale, 0.0).astype(jnp.bfloat16)
    high_scale = jnp.where(low, 0.0, scale).astype(jnp.bfloat16)
    low_one = jnp.where(low, 1.0, 0.0).astype(jnp.bfloat16)
    high_one = jnp.where(low, 0.0, 1.0).astype(jnp.bfloat16)
    for h in range(HEADS // 2):
        at = h * pair
        query = dot(normed, w_qkv_ref[:, at : at + pair]).astype(jnp.bfloat16)
        keys = dot(normed, w_qkv_ref[:, model + at : model + at + pair]).astype(jnp.bfloat16)
        values = dot(
            normed, w_qkv_ref[:, 2 * model + at : 2 * model + at + pair]
        ).astype(jnp.bfloat16)

        def attend(mask, own, other):
            scores = dot_nt(query * mask, keys)
            top = jnp.max(scores, axis=-1, keepdims=True)
            probs = jnp.exp(scores - top).astype(jnp.bfloat16)
            return dot(probs, values * own + other)

        first = attend(low_scale, low_one, high_one)
        second = attend(high_scale, high_one, low_one)
        total = pltpu.roll(jnp.where(low, second, first), head_dim, 1)
        mixed_ref[:, at : at + pair] = (jnp.where(low, first, second) / total).astype(jnp.bfloat16)
    resid = resid + dot(mixed_ref[...], w_out_ref[...])
    normed = layer_norm(resid, gains_ref[1:2, :]).astype(jnp.bfloat16)
    inner = jax.nn.gelu(dot(normed, w_up_ref[...])).astype(jnp.bfloat16)
    resid = resid + dot(inner, w_down_ref[...])
    final = layer_norm(resid, final_gain_ref[...])
    logits = jnp.sum(final * w_score_ref[...].astype(jnp.float32), axis=-1, keepdims=True)
    logits = jnp.transpose(jnp.broadcast_to(logits, (length, 128)))[0:1, :]
    shifted = logits - jnp.max(logits, axis=-1, keepdims=True)
    out_ref[pl.ds(slate, 1), :] = shifted - jnp.log(
        jnp.sum(jnp.exp(shifted), axis=-1, keepdims=True)
    )


def score_slates(
    position, rows, slates, length, w_in, w_qkv, w_out, w_up, w_down, norm_gains, final_gain, w_score
):
    width, model = w_in.shape
    whole = lambda a: pl.BlockSpec(a.shape, lambda i, *_: (0,) * a.ndim)
    operands = (
        rows,
        w_in,
        w_qkv[0],
        w_out[0],
        w_up[0],
        w_down[0],
        norm_gains[0],
        final_gain[None, :],
        w_score[None, :],
    )
    return pl.pallas_call(
        slate_kernel,
        grid_spec=pltpu.PrefetchScalarGridSpec(
            num_scalar_prefetch=1,
            grid=(slates,),
            in_specs=[whole(a) for a in operands],
            out_specs=pl.BlockSpec((slates, length), lambda i, *_: (0, 0)),
            scratch_shapes=[
                pltpu.VMEM(rows.shape, jnp.float32),
                pltpu.VMEM((length, width), jnp.float32),
                pltpu.VMEM((length, model), jnp.bfloat16),
            ],
        ),
        out_shape=jax.ShapeDtypeStruct((slates, length), jnp.float32),
        compiler_params=pltpu.CompilerParams(
            dimension_semantics=("arbitrary",), vmem_limit_bytes=56 * 1024 * 1024
        ),
        name="slates",
    )(position, *operands)


def per_device(
    candidate_owner,
    candidate_row,
    item_table,
    w_in,
    w_qkv,
    w_out,
    w_up,
    w_down,
    norm_gains,
    final_gain,
    w_score,
):
    slates, length, unused = candidate_owner.shape
    width = item_table.shape[1]
    shards = lax.axis_size(("gx", "gy"))
    capacity = max(2, 2 * slates * length // shards)
    outgoing, position = plan(candidate_owner[:, :, 0], candidate_row, shards, capacity)
    wanted = lax.all_to_all(outgoing, ("gx", "gy"), split_axis=0, concat_axis=0, tiled=True)
    found = item_table.at[wanted.reshape(-1)].get(mode="promise_in_bounds")
    found = found.reshape(shards, capacity, width)
    returned = lax.all_to_all(found, ("gx", "gy"), split_axis=0, concat_axis=0, tiled=True)
    return score_slates(
        position.reshape(-1),
        returned.reshape(shards * capacity, width),
        slates,
        length,
        w_in,
        w_qkv,
        w_out,
        w_up,
        w_down,
        norm_gains,
        final_gain,
        w_score,
    )


def solution(mesh):
    return jax.shard_map(
        per_device,
        mesh=mesh,
        in_specs=(
            P(("gx", "gy"), None, None),
            P(("gx", "gy"), None),
            P(("gx", "gy"), None),
            P(),
            P(),
            P(),
            P(),
            P(),
            P(),
            P(),
            P(),
        ),
        out_specs=P(("gx", "gy"), None),
        check_vma=False,
    )
```

```python
import functools

import jax
import jax.numpy as jnp
from jax import lax
from jax.experimental import pallas as pl
from jax.experimental.pallas import tpu as pltpu
from jax.sharding import PartitionSpec as P

HEADS = 8


def dot(a, b):
    return jnp.dot(a, b, preferred_element_type=jnp.float32)


def dot_nt(a, b):
    return lax.dot_general(a, b, (((1,), (1,)), ((), ())), preferred_element_type=jnp.float32)


def layer_norm(values, gain):
    mean = jnp.mean(values, axis=-1, keepdims=True)
    centred = values - mean
    variance = jnp.mean(centred * centred, axis=-1, keepdims=True)
    return centred * lax.rsqrt(variance + 1e-05) * gain


def cuts(total, parts):
    return [total * part // 8 for part in parts]


SLOT_PARTS = (0, 4, 8)
SLATE_PARTS = (0, 3, 8)


def plan_kernel(owner_ref, row_ref, outgoing_ref, position_ref, stage_ref, *, slot_cuts, slate_cuts):
    slates, length = row_ref.shape
    shards, unused, capacity = outgoing_ref.shape
    tri = (
        lax.broadcasted_iota(jnp.int32, (length, length), 0)
        <= lax.broadcasted_iota(jnp.int32, (length, length), 1)
    ).astype(jnp.float32).astype(jnp.bfloat16)
    shard_ids = lax.broadcasted_iota(jnp.int32, (shards, length), 0)
    slot_ids = lax.broadcasted_iota(jnp.int32, (capacity, length), 0)
    before = jnp.zeros((shards, 1), jnp.float32)
    acc = jnp.zeros((3 * shards, capacity), jnp.float32)
    for s in range(slates):
        owner = owner_ref[s]
        row = row_ref[s : s + 1, :]
        onehot = (owner == shard_ids).astype(jnp.float32)
        counts = dot(onehot.astype(jnp.bfloat16), tri) + before
        before = counts[:, length - 1 :]
        slot = (jnp.sum(counts * onehot, axis=0, keepdims=True) - 1.0).astype(jnp.int32)
        position = owner * slot_cuts[1] + slot
        for c in range(1, len(slot_cuts) - 1):
            low, high = slot_cuts[c], slot_cuts[c + 1]
            later = shards * low + owner * (high - low) + slot - low
            position = jnp.where(slot >= low, later, position)
        position_ref[s : s + 1, :] = position
        largest = jnp.max(slot, axis=-1, keepdims=True)
        stage = jnp.zeros((1, 128), jnp.int32)
        for c in range(1, len(slot_cuts) - 1):
            late = (largest >= slot_cuts[c]) | (s >= slate_cuts[c])
            stage = jnp.where(late, c, stage)
        stage_ref[s : s + 1, :] = stage
        digits = [(row & 255), ((row >> 8) & 255), (row >> 16)]
        lhs = jnp.concatenate(
            [onehot * digit.astype(jnp.float32) for digit in digits], axis=0
        ).astype(jnp.bfloat16)
        chosen = (slot == slot_ids).astype(jnp.float32).astype(jnp.bfloat16)
        acc = acc + dot_nt(lhs, chosen)
    parts = acc.astype(jnp.int32)
    outgoing_ref[:, 0, :] = (
        parts[:shards] + (parts[shards : 2 * shards] << 8) + (parts[2 * shards :] << 16)
    )


def plan(owner, row_index, shards, slot_cuts, slate_cuts):
    slates = row_index.shape[0]
    return pl.pallas_call(
        functools.partial(plan_kernel, slot_cuts=slot_cuts, slate_cuts=slate_cuts),
        out_shape=(
            jax.ShapeDtypeStruct((shards, 1, slot_cuts[-1]), jnp.int32),
            jax.ShapeDtypeStruct(row_index.shape, jnp.int32),
            jax.ShapeDtypeStruct((slates, 128), jnp.int32),
        ),
        name="plan",
    )(owner, row_index)


def stage_kernel(position_ref, stage_ref, *refs, number):
    row_refs, refs = refs[: number + 1], refs[number + 1 :]
    if number:
        done_ref, refs = refs[0], refs[1:]
        refs[-4][...] = done_ref[...]
    table_ref = refs[-3]
    start = 0
    for rows_ref in row_refs:
        count = rows_ref.shape[0]
        table_ref[start : start + count, :] = rows_ref[...].astype(jnp.float32)
        start += count

    def step(slate, carry):
        @pl.when(stage_ref[slate, 0] == number)
        def _():
            one_slate(slate, position_ref, *refs)

        return carry

    lax.fori_loop(0, stage_ref.shape[0], step, 0)


def one_slate(
    slate,
    position_ref,
    w_in_ref,
    w_qkv_ref,
    w_out_ref,
    w_up_ref,
    w_down_ref,
    gains_ref,
    final_gain_ref,
    w_score_ref,
    out_ref,
    table_ref,
    emb_ref,
    mixed_ref,
):
    length = emb_ref.shape[0]
    model = w_in_ref.shape[1]
    head_dim = model // HEADS
    pair = 2 * head_dim

    def pick(group, carry):
        for j in range(16):
            r = group * 16 + j
            p = position_ref[slate, r]
            emb_ref[pl.ds(r, 1), :] = table_ref[pl.ds(p, 1), :]
        return carry

    lax.fori_loop(0, length // 16, pick, 0)

    resid = dot(emb_ref[...].astype(jnp.bfloat16), w_in_ref[...])
    normed = layer_norm(resid, gains_ref[0:1, :]).astype(jnp.bfloat16)
    lane = lax.broadcasted_iota(jnp.int32, (1, pair), 1)
    low = lane < head_dim
    scale = head_dim ** (-0.5)
    low_scale = jnp.where(low, scale, 0.0).astype(jnp.bfloat16)
    high_scale = jnp.where(low, 0.0, scale).astype(jnp.bfloat16)
    low_one = jnp.where(low, 1.0, 0.0).astype(jnp.bfloat16)
    high_one = jnp.where(low, 0.0, 1.0).astype(jnp.bfloat16)
    for h in range(HEADS // 2):
        at = h * pair
        query = dot(normed, w_qkv_ref[:, at : at + pair]).astype(jnp.bfloat16)
        keys = dot(normed, w_qkv_ref[:, model + at : model + at + pair]).astype(jnp.bfloat16)
        values = dot(
            normed, w_qkv_ref[:, 2 * model + at : 2 * model + at + pair]
        ).astype(jnp.bfloat16)

        def attend(mask, own, other):
            scores = dot_nt(query * mask, keys)
            top = jnp.max(scores, axis=-1, keepdims=True)
            probs = jnp.exp(scores - top).astype(jnp.bfloat16)
            return dot(probs, values * own + other)

        first = attend(low_scale, low_one, high_one)
        second = attend(high_scale, high_one, low_one)
        total = pltpu.roll(jnp.where(low, second, first), head_dim, 1)
        mixed_ref[:, at : at + pair] = (jnp.where(low, first, second) / total).astype(jnp.bfloat16)
    resid = resid + dot(mixed_ref[...], w_out_ref[...])
    normed = layer_norm(resid, gains_ref[1:2, :]).astype(jnp.bfloat16)
    inner = jax.nn.gelu(dot(normed, w_up_ref[...])).astype(jnp.bfloat16)
    resid = resid + dot(inner, w_down_ref[...])
    final = layer_norm(resid, final_gain_ref[...])
    logits = jnp.sum(final * w_score_ref[...].astype(jnp.float32), axis=-1, keepdims=True)
    logits = jnp.transpose(jnp.broadcast_to(logits, (length, 128)))[0:1, :]
    shifted = logits - jnp.max(logits, axis=-1, keepdims=True)
    out_ref[pl.ds(slate, 1), :] = shifted - jnp.log(
        jnp.sum(jnp.exp(shifted), axis=-1, keepdims=True)
    )


def run_stage(number, position, stage, rows, done, weights, share):
    slates, length = position.shape
    w_in, w_qkv, w_out, w_up, w_down = weights[:5]
    width, model = w_in.shape
    total = sum(r.shape[0] for r in rows)
    smem = pl.BlockSpec(memory_space=pltpu.SMEM)
    vmem = pl.BlockSpec(memory_space=pltpu.VMEM)
    operands = (*rows, *([done] if number else []), *weights)
    matmuls = sum(w.size for w in (w_in, w_qkv, w_out, w_up, w_down))
    flops = 2 * length * (matmuls + 2 * length * model)
    return pl.pallas_call(
        functools.partial(stage_kernel, number=number),
        in_specs=[smem, smem] + [vmem] * len(operands),
        out_specs=vmem,
        scratch_shapes=[
            pltpu.VMEM((total, width), jnp.float32),
            pltpu.VMEM((length, width), jnp.float32),
            pltpu.VMEM((length, model), jnp.bfloat16),
        ],
        out_shape=jax.ShapeDtypeStruct((slates, length), jnp.float32),
        compiler_params=pltpu.CompilerParams(vmem_limit_bytes=56 * 1024 * 1024),
        cost_estimate=pl.CostEstimate(
            flops=share * flops,
            transcendentals=share * HEADS * length * length,
            bytes_accessed=2 * matmuls,
        ),
        name="stage" + str(number),
    )(position, stage, *operands)


def per_device(
    candidate_owner,
    candidate_row,
    item_table,
    w_in,
    w_qkv,
    w_out,
    w_up,
    w_down,
    norm_gains,
    final_gain,
    w_score,
):
    slates, length, unused = candidate_owner.shape
    width = item_table.shape[1]
    shards = lax.axis_size(("gx", "gy"))
    capacity = max(2, 2 * slates * length // shards)
    slot_cuts = cuts(capacity, SLOT_PARTS)
    slate_cuts = cuts(slates, SLATE_PARTS)
    owner = candidate_owner.reshape(slates, 1, length)
    outgoing, position, stage = plan(owner, candidate_row, shards, slot_cuts, slate_cuts)
    wanted = lax.all_to_all(outgoing, ("gx", "gy"), split_axis=0, concat_axis=0, tiled=True)
    wanted = wanted.reshape(shards, capacity)
    weights = (
        w_in,
        w_qkv[0],
        w_out[0],
        w_up[0],
        w_down[0],
        norm_gains[0],
        final_gain[None, :],
        w_score[None, :],
    )
    rows, scores = [], None
    for c in range(len(slot_cuts) - 1):
        size = slot_cuts[c + 1] - slot_cuts[c]
        index = wanted[:, slot_cuts[c] : slot_cuts[c + 1]].reshape(-1)
        found = item_table.at[index].get(mode="promise_in_bounds").reshape(shards, size, width)
        moved = lax.all_to_all(found, ("gx", "gy"), split_axis=0, concat_axis=0, tiled=True)
        rows.append(moved.reshape(shards * size, width))
    for c in range(len(rows)):
        share = slate_cuts[c + 1] - slate_cuts[c]
        scores = run_stage(c, position, stage, rows[: c + 1], scores, weights, share)
    return scores


def solution(mesh):
    return jax.shard_map(
        per_device,
        mesh=mesh,
        in_specs=(
            P(("gx", "gy"), None, None),
            P(("gx", "gy"), None),
            P(("gx", "gy"), None),
            P(),
            P(),
            P(),
            P(),
            P(),
            P(),
            P(),
            P(),
        ),
        out_specs=P(("gx", "gy"), None),
        check_vma=False,
    )
```
